32 devices in a mesh: row: 4 (over x, core), col: 8 (over z, y).
Axes of the slice: x: 2, y: 2, z: 4, core: 2. Of those that a mesh axis runs over, the one named last changes fastest.
Arguments:
- stored: float32 [16384, 16384], P('row', 'col'), as said below
Outputs:
- updated: float32 [16384, 16384], P('row', 'col')
- log_det: float32 [], replicated
Inputs may be any that keep to these rules, and one draw needn't show every extreme that they name: `stored`: read back into global order, the matrix is symmetric positive definite, with every eigenvalue at least 1.
All inputs are finite; a program needn't handle non-finite values.
Results may differ from the reference program's by a relative error of at most 0.0001.
Values sent between devices are 32-bit elements; how exact they have to be, the bound alone decides.
A program may use at most 256 MiB of HBM per device.

```python
import math
import jax
import jax.numpy as jnp
from jax import lax

N = 16384
NB = 512
PANELS = 2
N_ROW = 4
N_COL = 8


def to_storage(matrix):
    row_blocks = N // NB // N_ROW
    col_blocks = N // NB // N_COL
    shaped = matrix.reshape(row_blocks, N_ROW, NB, col_blocks, N_COL, NB)
    return shaped.transpose(1, 0, 2, 4, 3, 5).reshape(N, N)


def draw_stored(key, part):
    base_key = jax.random.fold_in(key, 7)
    first_key, second_key = jax.random.split(base_key)
    rank_count = N // 8
    factors = jax.random.normal(first_key, (N, rank_count), jnp.float32)
    weights = jnp.exp(jax.random.uniform(second_key, (rank_count,), jnp.float32, math.log(0.25), math.log(1.25)))
    scaled = factors * (weights / rank_count)[None, :]
    coupling = jnp.dot(scaled, factors.T, precision=lax.Precision.HIGHEST, preferred_element_type=jnp.float32)
    coupling = 0.5 * (coupling + coupling.T)
    return to_storage(coupling + jnp.eye(N, dtype=jnp.float32))


def setup_inputs(seed: int = 0) -> dict:
    key_of = jax.random.split(jax.random.key(seed), 2)
    stored = draw_stored(jax.random.fold_in(key_of[1], 71), 0)
    return dict(stored=stored)


def unpermute(stored):
    row_blocks = N // NB // N_ROW
    col_blocks = N // NB // N_COL
    shaped = stored.reshape(N_ROW, row_blocks, NB, N_COL, col_blocks, NB)
    return shaped.transpose(1, 0, 2, 4, 3, 5).reshape(N, N)

def permute(matrix):
    row_blocks = N // NB // N_ROW
    col_blocks = N // NB // N_COL
    shaped = matrix.reshape(row_blocks, N_ROW, NB, col_blocks, N_COL, NB)
    return shaped.transpose(1, 0, 2, 4, 3, 5).reshape(N, N)

def reference(stored):
    matrix = unpermute(stored)
    identity = jnp.eye(NB, dtype=jnp.float32)
    log_total = jnp.zeros((), jnp.float32)
    for number in range(PANELS):
        start = number * NB
        finish = start + NB
        factor = jnp.linalg.cholesky(matrix[start:finish, start:finish])
        inverse = jax.scipy.linalg.solve_triangular(factor, identity, lower=True)
        solved = jnp.dot(matrix[finish:, start:finish].astype(jnp.float32), inverse.T.astype(jnp.float32), precision=lax.Precision.HIGHEST, preferred_element_type=jnp.float32)
        log_total = log_total + 2.0 * jnp.sum(jnp.log(jnp.diagonal(factor)))
        update = jnp.dot(solved.astype(jnp.float32), solved.T.astype(jnp.float32), precision=lax.Precision.HIGHEST, preferred_element_type=jnp.float32)
        matrix = matrix.at[finish:, finish:].add(-update)
        matrix = matrix.at[start:finish, start:finish].set(factor)
        matrix = matrix.at[finish:, start:finish].set(solved)
        matrix = matrix.at[start:finish, finish:].set(0.0)
    return (permute(matrix), log_total)
```

```python
import functools

import jax
import jax.numpy as jnp
from jax import lax
from jax.experimental import pallas as pl
from jax.experimental.pallas import tpu as pltpu
from jax.sharding import PartitionSpec as P

NB = 512
PANELS = 2
BASE = 128
EXACT = lax.Precision.HIGHEST
SPLIT = lax.Precision.HIGH


def dot(a, b, dims, precision):
    return lax.dot_general(
        a, b, (dims, ((), ())), precision=precision, preferred_element_type=jnp.float32
    )


def factor_kernel(a_ref, l_ref, v_ref, work, aug):
    size = a_ref.shape[0]
    work[...] = a_ref[...]
    l_ref[...] = jnp.zeros_like(l_ref)
    v_ref[...] = jnp.zeros_like(v_ref)
    rows = lax.broadcasted_iota(jnp.int32, (BASE, BASE), 0)
    lanes = lax.broadcasted_iota(jnp.int32, (BASE, BASE), 1)
    row_ids = lax.broadcasted_iota(jnp.int32, (BASE, 1), 0)
    lane_ids = lax.broadcasted_iota(jnp.int32, (1, BASE), 1)
    for start in range(0, size, BASE):
        stop = start + BASE
        aug[:, :BASE] = work[start:stop, start:stop]
        aug[:, BASE:] = jnp.where(rows == lanes, 1.0, 0.0)

        def step(j, carry):
            row = aug[pl.ds(j, 1), :]
            pivot = jnp.sum(jnp.where(lane_ids == j, row[:, :BASE], 0.0), axis=1, keepdims=True)
            left = aug[:, :BASE]
            column = jnp.sum(jnp.where(lanes == j, left, 0.0), axis=1, keepdims=True)
            column = jnp.where(row_ids > j, column, 0.0)
            aug[...] = aug[...] - column * (row * (1.0 / pivot))
            return carry

        lax.fori_loop(0, BASE, step, 0)
        upper = aug[:, :BASE]
        pivots = jnp.sum(jnp.where(rows == lanes, upper, 0.0), axis=1, keepdims=True)
        scale = 1.0 / jnp.sqrt(pivots)
        lower = jnp.where(rows <= lanes, upper * scale, 0.0).T
        inverse = jnp.where(rows >= lanes, aug[:, BASE:] * scale, 0.0)
        l_ref[start:stop, start:stop] = lower
        v_ref[start:stop, start:stop] = inverse
        if start:
            mixed = dot(l_ref[start:stop, :start], v_ref[:start, :start], ((1,), (0,)), EXACT)
            v_ref[start:stop, :start] = -dot(inverse, mixed, ((1,), (0,)), EXACT)
        if stop < size:
            panel = dot(work[stop:, start:stop], inverse, ((1,), (1,)), EXACT)
            l_ref[stop:, start:stop] = panel
            work[stop:, stop:] = work[stop:, stop:] - dot(panel, panel, ((1,), (1,)), EXACT)


def factor_block(block):
    size = block.shape[0]
    shape = jax.ShapeDtypeStruct((size, size), jnp.float32)
    return pl.pallas_call(
        factor_kernel,
        out_shape=(shape, shape),
        in_specs=[pl.BlockSpec(memory_space=pltpu.VMEM)],
        out_specs=(pl.BlockSpec(memory_space=pltpu.VMEM),) * 2,
        scratch_shapes=[
            pltpu.VMEM((size, size), jnp.float32),
            pltpu.VMEM((BASE, 2 * BASE), jnp.float32),
        ],
        cost_estimate=pl.CostEstimate(
            flops=200 * 10**9 // 2, bytes_accessed=3 * 4 * size * size, transcendentals=0
        ),
    )(block)


def per_device(stored):
    row_count = lax.axis_size("row")
    col_count = lax.axis_size("col")
    row_index = lax.axis_index("row")
    col_index = lax.axis_index("col")
    local_rows, local_cols = stored.shape
    ratio = col_count // row_count
    piece = local_cols // row_count
    per_block = NB // piece
    corner = stored[:NB, :NB]

    def lead(row, col):
        return jnp.where((row_index == row) & (col_index == col), corner, 0.0)

    block00 = lax.psum(lead(0, 0), ("row", "col"))
    block1 = lax.psum(jnp.stack([lead(1, 0), lead(1, 1)]), ("row", "col"))
    block10, block11 = block1[0], block1[1]

    head = stored[:NB].reshape(NB, row_count, piece).transpose(1, 0, 2)
    swapped = lax.all_to_all(head, "row", 0, 0)
    mine = swapped[:PANELS].reshape(PANELS * NB, piece)
    pairs = []
    for q in range(row_count):
        for c in range(col_count):
            t, u = q // per_block, q % per_block
            target = (t * ratio + c // row_count) * per_block + u
            pairs.append((q * col_count + c, (c % row_count) * col_count + target))
    sent = lax.ppermute(mine, ("row", "col"), pairs)
    right_raw = lax.all_gather(mine, "row")
    left_raw = lax.all_gather(sent, "col")

    factor0, inverse0 = factor_block(block00)
    lower10 = dot(block10, inverse0, ((1,), (1,)), EXACT)
    factor1, inverse1 = factor_block(block11 - dot(lower10, lower10, ((1,), (1,)), EXACT))
    log_det = 2.0 * jnp.sum(jnp.log(jnp.diagonal(factor0)))
    log_det = log_det + 2.0 * jnp.sum(jnp.log(jnp.diagonal(factor1)))

    def solve(raw):
        raw0, raw1 = raw[:, :NB], raw[:, NB:]
        count = raw.shape[0] * raw.shape[2]
        first = jnp.einsum(
            "gkq,vk->gqv", raw0, inverse0, precision=SPLIT, preferred_element_type=jnp.float32
        ).reshape(count, NB)
        rest = raw1.transpose(0, 2, 1).reshape(count, NB) - dot(first, lower10, ((1,), (1,)), SPLIT)
        return first, dot(rest, inverse1, ((1,), (1,)), SPLIT)

    row_block = (jnp.arange(local_rows, dtype=jnp.int32) // NB * row_count + row_index)[:, None]
    left0, left1 = solve(left_raw)
    right0, right1 = solve(right_raw)
    left = jnp.concatenate([left0, left1], axis=1)
    right = jnp.concatenate([right0, right1], axis=1)
    trailing = stored - dot(left, right, ((1,), (1,)), SPLIT)
    matrix = jnp.where(row_block < PANELS, 0.0, trailing)

    tile = lambda block: jnp.tile(block, (local_rows // NB, 1))
    panel0 = jnp.where(
        row_block == 0, tile(factor0), jnp.where(row_block == 1, tile(lower10), left0)
    )
    panel1 = jnp.where(
        row_block == 0, 0.0, jnp.where(row_block == 1, tile(factor1), left1)
    )
    column = jnp.where(
        col_index == 0, panel0, jnp.where(col_index == 1, panel1, matrix[:, :NB])
    )
    return matrix.at[:, :NB].set(column), log_det


def solution(mesh):
    placed = (P("row", "col"),)
    return jax.shard_map(
        per_device, mesh=mesh, in_specs=placed, out_specs=(P("row", "col"), P()), check_vma=False
    )
```
